256 devices in a mesh: vocab: 64 (over y, z, core), section: 4 (over x).
Axes of the slice: x: 4, y: 4, z: 8, core: 2. Of those that a mesh axis runs over, the one named last changes fastest.
Arguments:
- hidden: bfloat16 [4, 256, 8192], P('section', 'vocab'), may hold values from -64 to 64
- policy_head: bfloat16 [76032, 8192], P(('vocab', 'section')), may hold values from -1 to 1
- reference_head: bfloat16 [76032, 8192], P(('vocab', 'section')), may hold values from -1 to 1
- targets: int32 [4, 256], replicated, may hold values from 0 to 76031
- loss_mask: int32 [4, 256], replicated, may hold values 0 or 1
Outputs:
- token_logprob: float32 [4, 256], replicated
- token_kl: float32 [4, 256], replicated
- totals: float32 [3], replicated
The draws below stay inside these ranges and needn't reach their ends.
All inputs are finite; a program needn't handle non-finite values.
Results may differ from the reference program's by a relative error of at most 0.0003.
Values may be sent and summed in bfloat16 or wider, within the bound.
No kernel may reach another device: no remote copies, remote signals or barrier semaphores. Data moves between devices by JAX's collectives and lax.ppermute only.
A program may use at most 128 MiB of HBM per device.

```python
import jax
import jax.numpy as jnp
from jax import lax

D = 8192
VOCAB = 76032
TOK_MB = 256
MICRO = 4


def head_row(key, salt, index):
    base = jax.random.fold_in(jax.random.fold_in(key, salt), index)
    return jax.random.truncated_normal(base, -6.0, 6.0, (D,), jnp.float32) * D ** (-0.5)


def head_rows(key, salt):
    indices = jnp.arange(VOCAB, dtype=jnp.int32)
    return jax.vmap(lambda index: head_row(key, salt, index))(indices)


def draw_policy_head(key, part):
    return head_rows(key, 11).astype(jnp.bfloat16)


def draw_reference_head(key, part):
    return (head_rows(key, 11) + 0.6 * head_rows(key, 12)).astype(jnp.bfloat16)


def draw_hidden(key, part):
    values = jax.random.truncated_normal(jax.random.fold_in(key, 21), -6.0, 6.0, (MICRO, TOK_MB, D), jnp.float32)
    return values.astype(jnp.bfloat16)


def touch_ends(values, stream_key, smallest, high):
    longest = values.shape.index(max(values.shape))
    spots = []
    for shift in (0, 1):
        where = [jax.random.randint(jax.random.fold_in(stream_key, axis), (), 0, length) for axis, length in enumerate(values.shape)]
        where[longest] = (where[longest] + shift) % values.shape[longest]
        spots.append(tuple(where))
    return values.at[spots[0]].set(smallest).at[spots[1]].set(high)


def setup_inputs(seed: int = 0) -> dict:
    streams_of = jax.random.split(jax.random.key(seed), 6)
    return {
        "hidden": draw_hidden(jax.random.fold_in(streams_of[5], 71), 0),
        "policy_head": draw_policy_head(jax.random.fold_in(streams_of[5], 71), 0),
        "reference_head": draw_reference_head(jax.random.fold_in(streams_of[5], 71), 0),
        "targets": touch_ends(jax.random.randint(streams_of[3], (MICRO, TOK_MB), 0, VOCAB), jax.random.fold_in(streams_of[3], 1), 0, VOCAB - 1).astype(jnp.int32),
        "loss_mask": touch_ends((jax.random.randint(streams_of[4], (MICRO, TOK_MB), 0, 4) < 3).astype(jnp.int32), jax.random.fold_in(streams_of[4], 1), 0, 1),
    }


def log_norm(logits):
    largest = jnp.max(logits, axis=1, keepdims=True)
    return largest[:, 0] + jnp.log(jnp.sum(jnp.exp(logits - largest), axis=1))


def micro_batch(inputs, policy_head, reference_head):
    hidden_rows, target = inputs
    contract_dims = (((1,), (1,)), ((), ()))
    policy_logits = lax.dot_general(hidden_rows, policy_head, contract_dims, preferred_element_type=jnp.float32)
    refer_logits = lax.dot_general(hidden_rows, reference_head, contract_dims, preferred_element_type=jnp.float32)
    policy_lse = log_norm(policy_logits)
    refer_lse = log_norm(refer_logits)
    policy_probs = jnp.exp(policy_logits - policy_lse[:, None])
    chosen = jnp.take_along_axis(policy_logits, target[:, None].astype(jnp.int32), axis=1)[:, 0]
    logprob = chosen - policy_lse
    entropy = policy_lse - jnp.sum(policy_probs * policy_logits, axis=1)
    divergence = jnp.sum(policy_probs * (policy_logits - refer_logits), axis=1) - policy_lse + refer_lse
    return logprob, entropy, divergence


def reference(hidden, policy_head, reference_head, targets, loss_mask):
    logprob, entropy, divergence = lax.map(lambda inputs: micro_batch(inputs, policy_head, reference_head), (hidden, targets))
    weights = loss_mask.astype(jnp.float32)
    scale = 1.0 / (hidden.shape[0] * hidden.shape[1])
    totals = jnp.stack([jnp.sum(weights * logprob), jnp.sum(weights * entropy), jnp.sum(weights * divergence)]) * scale
    return logprob, divergence, totals
```

```python
import functools

import jax
import jax.numpy as jnp
from jax import lax
from jax.experimental import pallas as pl
from jax.experimental.pallas import tpu as pltpu
from jax.sharding import Mesh
from jax.sharding import PartitionSpec as P

ROWS = ("y", "z", "core", "x")
MASKED = -1e30


def shifted(array, axis, step):
    count = lax.axis_size(axis)
    return lax.ppermute(array, axis, [((k + step) % count, k) for k in range(count)])


def ordered_z_kernel(place, *refs):
    pieces, low, high, staged = refs[:-3], refs[-3], refs[-2], refs[-1]
    count = len(pieces)
    rows = pieces[0].shape[0]
    for k, piece in enumerate(pieces):
        at = lax.rem(place[0] + k, count)
        staged[at] = piece[...].astype(jnp.float32)
    half = count // 2
    whole = staged[...].reshape(count * rows, -1).astype(low.dtype)
    low[...] = whole[: half * rows]
    high[...] = whole[half * rows :]


def ordered_z(pieces, place):
    count, (rows, width) = len(pieces), pieces[0].shape
    half = jax.ShapeDtypeStruct((count * rows // 2, width), pieces[0].dtype)
    return pl.pallas_call(
        ordered_z_kernel,
        out_shape=(half, half),
        in_specs=[pl.BlockSpec(memory_space=pltpu.SMEM)]
        + [pl.BlockSpec(memory_space=pltpu.VMEM)] * count,
        out_specs=(pl.BlockSpec(memory_space=pltpu.VMEM),) * 2,
        scratch_shapes=[pltpu.VMEM((count, rows, width), jnp.float32)],
        compiler_params=pltpu.CompilerParams(vmem_limit_bytes=8 * 2**20),
        name="ordered_z",
    )(place.reshape(1), *pieces)


def ordered_kernel(place, *refs):
    pieces, halves, out = refs[:-3], refs[-3:-1], refs[-1]
    for k, piece in enumerate(pieces):
        out[lax.rem(place[0] + k, len(pieces))] = piece[...]
    for k, half in enumerate(halves):
        size = out.shape[0] // 2
        half[...] = out[k * size : (k + 1) * size].reshape(half.shape)


def ordered(pieces, place):
    count, (rows, width) = len(pieces), pieces[0].shape
    half = jax.ShapeDtypeStruct((count * rows // 2, width), pieces[0].dtype)
    return pl.pallas_call(
        ordered_kernel,
        out_shape=(half, half),
        in_specs=[pl.BlockSpec(memory_space=pltpu.SMEM)]
        + [pl.BlockSpec(memory_space=pltpu.VMEM)] * count,
        out_specs=(pl.BlockSpec(memory_space=pltpu.VMEM),) * 2,
        scratch_shapes=[pltpu.VMEM((count, rows, width), pieces[0].dtype)],
        compiler_params=pltpu.CompilerParams(vmem_limit_bytes=6 * 2**20),
        name="ordered",
    )(place.reshape(1), *pieces)


def moments_of(policy, refer, wanted, first_row, valid):
    rows = lax.broadcasted_iota(jnp.int32, policy.shape, 0)
    real = rows < valid
    policy = jnp.where(real, policy, MASKED)
    refer = jnp.where(real, refer, MASKED)
    top = jnp.max(policy, axis=0, keepdims=True)
    shift = policy - top
    power = jnp.exp(shift)
    rtop = jnp.max(refer, axis=0, keepdims=True)
    total = jnp.sum(power, axis=0, keepdims=True)
    first = jnp.sum(jnp.where(real, power * shift, 0.0), axis=0, keepdims=True)
    cross = jnp.sum(jnp.where(real, power * (policy - refer), 0.0), axis=0, keepdims=True)
    hit = jnp.logical_and(rows + first_row == wanted, real)
    chosen = jnp.sum(jnp.where(hit, policy, 0.0), axis=0, keepdims=True)
    rtotal = jnp.sum(jnp.exp(refer - rtop), axis=0, keepdims=True)
    return top, total, first, cross, chosen, rtop, rtotal


def merge_many(moments):
    top = functools.reduce(jnp.maximum, [m[0] for m in moments])
    rtop = functools.reduce(jnp.maximum, [m[5] for m in moments])
    total = first = cross = chosen = rtotal = 0.0
    for m in moments:
        down = m[0] - top
        factor = jnp.exp(down)
        total += factor * m[1]
        first += factor * (m[2] + down * m[1])
        cross += factor * m[3]
        chosen += m[4]
        rtotal += jnp.exp(m[5] - rtop) * m[6]
    return top, total, first, cross, chosen, rtop, rtotal


def moments_kernel(slots, valid, numbers, wanted_ref, *refs):
    hidden, heads = refs[: len(slots)], refs[len(slots) : len(slots) + 4]
    out, sums = refs[-2], refs[-1]
    step = pl.program_id(0)
    tokens = jnp.concatenate([piece[...] for piece in hidden], axis=0)

    @pl.when(step == 0)
    def _():
        sums[...] = jnp.zeros_like(sums)
        if len(refs) > len(slots) + 6:
            out[...] = refs[len(slots) + 4][...]

    for k, head in enumerate(heads):
        sums[k] += lax.dot_general(
            head[...], tokens, (((1,), (1,)), ((), ())), preferred_element_type=jnp.float32
        )

    @pl.when(step == pl.num_programs(0) - 1)
    def _():
        spans, at = [], 0
        for (number, lane), piece in zip(slots, hidden):
            width = piece.shape[0]
            row = wanted_ref[pl.ds(numbers[number], 1), :]
            spans.append((at, width, number, lane, row[:, lane : lane + width]))
            at += width
        wanted = jnp.concatenate([span[-1] for span in spans], axis=1)
        found = [
            moments_of(sums[k], sums[k + 1], wanted, numbers[k // 2], valid) for k in (0, 2)
        ]
        merged = merge_many(found)
        merged = jnp.concatenate([*merged, jnp.zeros_like(merged[0])], axis=0)
        for at, width, number, lane, _ in spans:
            out[numbers[number], :, lane : lane + width] = merged[:, at : at + width]


def moments_call(slots, pieces, heads, numbers, wanted, before, depth):
    rows, width = heads[0].shape
    padded = -(-rows // 16) * 16
    count = sum(piece.shape[0] for piece in pieces)
    extra = [] if before is None else [before]
    out = jax.ShapeDtypeStruct((4, 8, 128), jnp.float32)
    whole = pl.BlockSpec((4, 8, 128), lambda k: (0, 0, 0))
    return pl.pallas_call(
        functools.partial(moments_kernel, slots, rows),
        grid=(width // depth,),
        out_shape=out,
        in_specs=[
            pl.BlockSpec(memory_space=pltpu.SMEM),
            pl.BlockSpec(wanted.shape, lambda k: (0, 0)),
        ]
        + [pl.BlockSpec((piece.shape[0], depth), lambda k: (0, k)) for piece in pieces]
        + [pl.BlockSpec((padded, depth), lambda k: (0, k))] * 4
        + [whole] * len(extra),
        out_specs=whole,
        scratch_shapes=[pltpu.VMEM((4, padded, count), jnp.float32)],
        compiler_params=pltpu.CompilerParams(vmem_limit_bytes=24 * 2**20),
        name="moments",
    )(numbers, wanted, *pieces, *heads, *extra)


def received(array, axis):
    count = lax.psum(1, axis)
    return lax.all_to_all(
        jnp.broadcast_to(array[None], (count, *array.shape)), axis, 0, 0, tiled=True
    )


def combined(pieces):
    merged = merge_many([tuple(piece[:, r] for r in range(7)) for piece in pieces])
    return jnp.stack([*merged, jnp.zeros_like(merged[0])], axis=1)


def finished_kernel(pieces, weights, out):
    merged = merge_many(
        [tuple(pieces[k, :, r, :] for r in range(7)) for k in range(pieces.shape[0])]
    )
    top, total, first, cross, chosen, rtop, rtotal = merged
    scale = jnp.log(total)
    policy_lse = top + scale
    refer_lse = rtop + jnp.log(rtotal)
    logprob = chosen - policy_lse
    entropy = scale - first / total
    divergence = cross / total - policy_lse + refer_lse
    out[0], out[1] = logprob, divergence
    for k, part in enumerate((logprob, entropy, divergence)):
        out[2, k : k + 1, :] = jnp.sum(weights[...] * part, axis=0, keepdims=True)
    out[2, 3:4, :] = jnp.zeros((1, out.shape[2]), out.dtype)


def finished(pieces, weights):
    return pl.pallas_call(
        finished_kernel,
        out_shape=jax.ShapeDtypeStruct((3, 4, 128), jnp.float32),
        compiler_params=pltpu.CompilerParams(vmem_limit_bytes=4 * 2**20),
        name="finished",
    )(pieces, weights)


def placed_kernel(size, core, here, there, logprob, divergence, totals):
    first = core[0] == 0
    low_x = lax.broadcasted_iota(jnp.int32, (4, 64), 1) // 16
    own_x = low_x == lax.broadcasted_iota(jnp.int32, (4, 64), 0)
    columns = lax.broadcasted_iota(jnp.int32, (64, 256), 1)
    source = lax.broadcasted_iota(jnp.int32, (64, 256), 0)
    within = (source % 16) // 4 * 8 + source % 4
    rows, maps = [], []
    for index in range(2):
        both = [jnp.where(first, here[k], there[k]) for k in range(2)]
        if index == 1:
            both = [jnp.where(first, there[k], here[k]) for k in range(2)]
        for y in range(4):
            rows.append(
                jnp.concatenate([jnp.where(own_x, part[y : y + 1, :64], 0.0) for part in both], 0)
            )
            maps.append(columns == within + (y * 64 + index * 4))
        rows.append(jnp.concatenate([part[:, 64:] for part in both], 0))
        maps.append(columns == source // 16 * 64 + 32 + within + index * 4)
    result = jnp.zeros((8, 256), jnp.float32)
    for row, chosen in zip(rows, maps):
        result += lax.dot_general(
            row,
            chosen.astype(jnp.float32),
            (((1,), (0,)), ((), ())),
            precision=lax.Precision.HIGHEST,
            preferred_element_type=jnp.float32,
        )
    logprob[...] = result[:4]
    divergence[...] = result[4:]
    for k in range(3):
        totals[k] = jnp.sum(here[2, k : k + 1, :] + there[2, k : k + 1, :]) / size


def placed(here, there, core, size):
    whole = jax.ShapeDtypeStruct((4, 256), jnp.float32)
    vmem = pl.BlockSpec(memory_space=pltpu.VMEM)
    smem = pl.BlockSpec(memory_space=pltpu.SMEM)
    return pl.pallas_call(
        functools.partial(placed_kernel, size),
        out_shape=(whole, whole, jax.ShapeDtypeStruct((3,), jnp.float32)),
        in_specs=[smem, vmem, vmem],
        out_specs=(vmem, vmem, smem),
        compiler_params=pltpu.CompilerParams(vmem_limit_bytes=4 * 2**20),
        name="placed",
    )(core.reshape(1), here, there)


def by_slot(array):
    low = array[:, :, :4].transpose(1, 0, 2, 3).reshape(4, 64)
    high = array[:, :, 4:].reshape(4, 64)
    return jnp.concatenate([low, high], axis=1)


def on_device(hidden, policy_head, reference_head, targets, loss_mask):
    x, y, z, core = (lax.axis_index(name) for name in ("x", "y", "z", "core"))
    rows = policy_head.shape[0]
    heads = [policy_head, reference_head]
    heads += [shifted(head, "core", 1) for head in heads]
    numbers = jnp.stack(
        [
            (((y * 8 + z) * 2 + core) * 4 + x) * rows,
            (((y * 8 + z) * 2 + 1 - core) * 4 + x) * rows,
            y,
            (y + 1) % 4,
            (y + 3) % 4,
            (y + 2) % 4,
            x,
            (x + 1) % 4,
            (x + 3) % 4,
            (x + 2) % 4,
        ]
    ).astype(jnp.int32)
    mine = lambda array: lax.dynamic_index_in_dim(
        array.reshape(4, 4, 8, 2, 4), core, axis=3, keepdims=False
    )
    wanted = by_slot(mine(targets))
    weights = by_slot(mine(loss_mask)).astype(jnp.float32)

    own = hidden[0]
    up = [own]
    down = [own]
    for k in range(4):
        up.append(shifted(up[-1], "z", 1))
        if k < 3:
            down.append(shifted(down[-1], "z", -1))
    low, high = ordered_z([*up, *down[:0:-1]], z)
    one = ordered([low] + [shifted(low, "x", k) for k in (1, 2, 3)], x)
    two = ordered([high] + [shifted(high, "y", k) for k in (1, 2, 3)], y)

    one_up, one_down = [shifted(one[0], "y", 1)], [shifted(one[1], "y", -1)]
    two_up, two_down = [shifted(two[0], "x", 1)], [shifted(two[1], "x", -1)]
    one_up.append(shifted(one[1], "y", 1))
    one_down.append(shifted(one[0], "y", -1))
    two_up.append(shifted(two[1], "x", 1))
    two_down.append(shifted(two[0], "x", -1))
    one_far = [shifted(one_up[0], "y", 1), shifted(one_down[0], "y", -1)]
    two_far = [shifted(two_up[0], "x", 1), shifted(two_down[0], "x", -1)]

    early = ((2, 0), (2, 32), (6, 64), (6, 96), (3, 0), (4, 32), (7, 64), (8, 96))
    late = ((3, 32), (4, 0), (7, 96), (8, 64), (5, 0), (5, 32), (9, 64), (9, 96))
    pieces = [*one, *two, one_up[0], one_down[0], two_up[0], two_down[0]]
    moments = moments_call(early, pieces, heads, numbers, wanted, None, 2048)
    pieces = [one_up[1], one_down[1], two_up[1], two_down[1], *one_far, *two_far]
    moments = moments_call(late, pieces, heads, numbers, wanted, moments, 2048)

    moments = combined(received(moments, ("y", "x")))
    here = finished(received(moments, "z"), weights)
    there = shifted(here, "core", 1)
    logprob, divergence, totals = placed(here, there, core, targets.size)
    return logprob, divergence, totals


def solution(mesh):
    torus = Mesh(mesh.devices.reshape(4, 8, 2, 4), ROWS)
    placed = (P("x", ("y", "z", "core"), None), P(ROWS, None), P(ROWS, None), P(), P())
    return jax.shard_map(
        on_device, mesh=torus, in_specs=placed, out_specs=(P(), P(), P()), check_vma=False
    )
```

```python
import functools

import jax
import jax.numpy as jnp
from jax import lax
from jax.experimental import pallas as pl
from jax.experimental.pallas import tpu as pltpu
from jax.sharding import Mesh
from jax.sharding import PartitionSpec as P

ROWS = ("y", "z", "core", "x")
MASKED = -1e30


def shifted(array, axis, step):
    count = lax.axis_size(axis)
    return lax.ppermute(array, axis, [((k + step) % count, k) for k in range(count)])


def ordered_z_kernel(place, *refs):
    pieces, low, high, staged = refs[:-3], refs[-3], refs[-2], refs[-1]
    count = len(pieces)
    rows = pieces[0].shape[0]
    for k, piece in enumerate(pieces):
        at = lax.rem(place[0] + k, count)
        staged[at] = piece[...].astype(jnp.float32)
    half = count // 2
    whole = staged[...].reshape(count * rows, -1).astype(low.dtype)
    low[...] = whole[: half * rows]
    high[...] = whole[half * rows :]


def ordered_z(pieces, place):
    count, (rows, width) = len(pieces), pieces[0].shape
    half = jax.ShapeDtypeStruct((count * rows // 2, width), pieces[0].dtype)
    return pl.pallas_call(
        ordered_z_kernel,
        out_shape=(half, half),
        in_specs=[pl.BlockSpec(memory_space=pltpu.SMEM)]
        + [pl.BlockSpec(memory_space=pltpu.VMEM)] * count,
        out_specs=(pl.BlockSpec(memory_space=pltpu.VMEM),) * 2,
        scratch_shapes=[pltpu.VMEM((count, rows, width), jnp.float32)],
        compiler_params=pltpu.CompilerParams(vmem_limit_bytes=8 * 2**20),
        name="ordered_z",
    )(place.reshape(1), *pieces)


def ordered_kernel(place, *refs):
    pieces, halves, out = refs[:-3], refs[-3:-1], refs[-1]
    for k, piece in enumerate(pieces):
        out[lax.rem(place[0] + k, len(pieces))] = piece[...]
    for k, half in enumerate(halves):
        size = out.shape[0] // 2
        half[...] = out[k * size : (k + 1) * size].reshape(half.shape)


def ordered(pieces, place):
    count, (rows, width) = len(pieces), pieces[0].shape
    half = jax.ShapeDtypeStruct((count * rows // 2, width), pieces[0].dtype)
    return pl.pallas_call(
        ordered_kernel,
        out_shape=(half, half),
        in_specs=[pl.BlockSpec(memory_space=pltpu.SMEM)]
        + [pl.BlockSpec(memory_space=pltpu.VMEM)] * count,
        out_specs=(pl.BlockSpec(memory_space=pltpu.VMEM),) * 2,
        scratch_shapes=[pltpu.VMEM((count, rows, width), pieces[0].dtype)],
        compiler_params=pltpu.CompilerParams(vmem_limit_bytes=6 * 2**20),
        name="ordered",
    )(place.reshape(1), *pieces)


def moments_of(policy, refer, wanted, first_row, valid):
    rows = lax.broadcasted_iota(jnp.int32, policy.shape, 0)
    real = rows < valid
    policy = jnp.where(real, policy, MASKED)
    refer = jnp.where(real, refer, MASKED)
    top = jnp.max(policy, axis=0, keepdims=True)
    shift = policy - top
    power = jnp.exp(shift)
    rtop = jnp.max(refer, axis=0, keepdims=True)
    total = jnp.sum(power, axis=0, keepdims=True)
    first = jnp.sum(jnp.where(real, power * shift, 0.0), axis=0, keepdims=True)
    cross = jnp.sum(jnp.where(real, power * (policy - refer), 0.0), axis=0, keepdims=True)
    hit = jnp.logical_and(rows + first_row == wanted, real)
    chosen = jnp.sum(jnp.where(hit, policy, 0.0), axis=0, keepdims=True)
    rtotal = jnp.sum(jnp.exp(refer - rtop), axis=0, keepdims=True)
    return top, total, first, cross, chosen, rtop, rtotal


def merge_many(moments):
    top = functools.reduce(jnp.maximum, [m[0] for m in moments])
    rtop = functools.reduce(jnp.maximum, [m[5] for m in moments])
    total = first = cross = chosen = rtotal = 0.0
    for m in moments:
        down = m[0] - top
        factor = jnp.exp(down)
        total += factor * m[1]
        first += factor * (m[2] + down * m[1])
        cross += factor * m[3]
        chosen += m[4]
        rtotal += jnp.exp(m[5] - rtop) * m[6]
    return top, total, first, cross, chosen, rtop, rtotal


def moments_kernel(slots, copies, first, numbers, wanted_ref, *refs):
    hidden, heads, refs = refs[: len(slots)], refs[len(slots) : len(slots) + 4], refs[len(slots) + 4 :]
    out, sums, ready = refs[-3:]
    copied, held = refs[-8 if first else -4], refs[-7:-3] if first else heads
    valid, width = heads[0].shape
    padded = sums.shape[1]
    blank = jnp.zeros((padded - valid, 256), heads[0].dtype)
    if first:
        loads = [
            pltpu.make_async_copy(head, held[k], ready.at[k]) for k, head in enumerate(heads)
        ]
        for load in loads:
            load.start()
    else:
        out[...] = refs[0][...]

    def multiply(*totals):
        for h in range(4):
            if first:
                loads[h].wait()
            for at in range(0, width, 512):
                for unit in range(2):
                    span = slice(at + unit * 256, at + unit * 256 + 256)
                    tokens = jnp.concatenate([piece[:, span] for piece in hidden], axis=0)
                    rows = jnp.concatenate([held[h][:, span], blank], axis=0)
                    pltpu.matmul_push_rhs(tokens, at // 512 % 2, unit, transpose=True)
                    pltpu.matmul_acc_lhs(
                        totals[2 * (h % 2) + unit], rows, load_staged_rhs=at // 512 % 2
                    )
            sums[h] = pltpu.matmul_pop(totals[2 * (h % 2)]) + pltpu.matmul_pop(
                totals[2 * (h % 2) + 1]
            )

    pl.run_scoped(multiply, *[pltpu.ACC(k % 2)((padded, 256), jnp.float32) for k in range(4)])

    spans, at = [], 0
    for (number, lane), piece in zip(slots, hidden):
        count = piece.shape[0]
        row = wanted_ref[pl.ds(numbers[number], 1), :]
        spans.append((at, count, number, lane, row[:, lane : lane + count]))
        at += count
    wanted = jnp.concatenate([span[-1] for span in spans], axis=1)
    found = [moments_of(sums[k], sums[k + 1], wanted, numbers[k // 2], valid) for k in (0, 2)]
    for r, part in enumerate(merge_many(found)):
        for at, count, number, lane, _ in spans:
            out[r, pl.ds(numbers[number], 1), lane : lane + count] = part[:, at : at + count]
    out[7] = jnp.zeros_like(out[7])
    for k in range(copies):
        copied[k] = out[...]


def moments_call(slots, pieces, heads, numbers, wanted, before, copies):
    rows, width = heads[0].shape
    padded = -(-rows // 16) * 16
    vmem = pl.BlockSpec(memory_space=pltpu.VMEM)
    hbm = pl.BlockSpec(memory_space=pltpu.HBM)
    first = before is None
    held = [jax.ShapeDtypeStruct(head.shape, head.dtype) for head in heads] if first else []
    return pl.pallas_call(
        functools.partial(moments_kernel, slots, copies, first),
        out_shape=(jax.ShapeDtypeStruct((copies, 8, 4, 128), jnp.float32), *held),
        in_specs=[pl.BlockSpec(memory_space=pltpu.SMEM), vmem]
        + [vmem] * len(pieces)
        + [hbm if first else vmem] * 4
        + ([] if first else [vmem]),
        out_specs=(vmem,) * (1 + len(held)),
        scratch_shapes=[
            pltpu.VMEM((8, 4, 128), jnp.float32),
            pltpu.VMEM((4, padded, 256), jnp.float32),
            pltpu.SemaphoreType.DMA((4,)),
        ],
        compiler_params=pltpu.CompilerParams(vmem_limit_bytes=(28 if first else 12) * 2**20),
        name="moments",
    )(numbers, wanted, *pieces, *heads, *([] if first else [before[0]]))


def received(array, axis):
    return lax.all_to_all(array, axis, 0, 0, tiled=True)


def combined_kernel(pieces, out):
    merged = merge_many([tuple(pieces[k, r] for r in range(7)) for k in range(pieces.shape[0])])
    for k in range(out.shape[0]):
        for r, part in enumerate(merged):
            out[k, r] = part
        out[k, 7] = jnp.zeros_like(merged[0])


def combined(pieces, copies):
    return pl.pallas_call(
        combined_kernel,
        out_shape=jax.ShapeDtypeStruct((copies, *pieces.shape[1:]), pieces.dtype),
        compiler_params=pltpu.CompilerParams(vmem_limit_bytes=4 * 2**20),
        name="combined",
    )(pieces)


def finished_kernel(pieces, weights, out):
    merged = merge_many([tuple(pieces[k, r] for r in range(7)) for k in range(pieces.shape[0])])
    top, total, first, cross, chosen, rtop, rtotal = merged
    scale = jnp.log(total)
    policy_lse = top + scale
    refer_lse = rtop + jnp.log(rtotal)
    logprob = chosen - policy_lse
    entropy = scale - first / total
    divergence = cross / total - policy_lse + refer_lse
    out[0], out[1] = logprob, divergence
    for k, part in enumerate((logprob, entropy, divergence)):
        out[2, k : k + 1, :] = jnp.sum(weights[...] * part, axis=0, keepdims=True)
    out[2, 3:4, :] = jnp.zeros((1, out.shape[2]), out.dtype)


def finished(pieces, weights):
    return pl.pallas_call(
        finished_kernel,
        out_shape=jax.ShapeDtypeStruct((3, 4, 128), jnp.float32),
        compiler_params=pltpu.CompilerParams(vmem_limit_bytes=4 * 2**20),
        name="finished",
    )(pieces, weights)


def placed_kernel(size, core, here, there, logprob, divergence, totals):
    first = core[0] == 0
    low_x = lax.broadcasted_iota(jnp.int32, (4, 64), 1) // 16
    own_x = low_x == lax.broadcasted_iota(jnp.int32, (4, 64), 0)
    columns = lax.broadcasted_iota(jnp.int32, (64, 256), 1)
    source = lax.broadcasted_iota(jnp.int32, (64, 256), 0)
    within = (source % 16) // 4 * 8 + source % 4
    rows, maps = [], []
    for index in range(2):
        both = [jnp.where(first, here[k], there[k]) for k in range(2)]
        if index == 1:
            both = [jnp.where(first, there[k], here[k]) for k in range(2)]
        for y in range(4):
            rows.append(
                jnp.concatenate([jnp.where(own_x, part[y : y + 1, :64], 0.0) for part in both], 0)
            )
            maps.append(columns == within + (y * 64 + index * 4))
        rows.append(jnp.concatenate([part[:, 64:] for part in both], 0))
        maps.append(columns == source // 16 * 64 + 32 + within + index * 4)
    result = jnp.zeros((8, 256), jnp.float32)
    for row, chosen in zip(rows, maps):
        result += lax.dot_general(
            row,
            chosen.astype(jnp.float32),
            (((1,), (0,)), ((), ())),
            precision=lax.Precision.HIGHEST,
            preferred_element_type=jnp.float32,
        )
    logprob[...] = result[:4]
    divergence[...] = result[4:]
    for k in range(3):
        totals[k] = jnp.sum(here[2, k : k + 1, :] + there[2, k : k + 1, :]) / size


def placed(here, there, core, size):
    whole = jax.ShapeDtypeStruct((4, 256), jnp.float32)
    vmem = pl.BlockSpec(memory_space=pltpu.VMEM)
    smem = pl.BlockSpec(memory_space=pltpu.SMEM)
    return pl.pallas_call(
        functools.partial(placed_kernel, size),
        out_shape=(whole, whole, jax.ShapeDtypeStruct((3,), jnp.float32)),
        in_specs=[smem, vmem, vmem],
        out_specs=(vmem, vmem, smem),
        compiler_params=pltpu.CompilerParams(vmem_limit_bytes=4 * 2**20),
        name="placed",
    )(core.reshape(1), here, there)


def by_slot(array):
    low = array[:, :, :4].transpose(1, 0, 2, 3).reshape(4, 64)
    high = array[:, :, 4:].reshape(4, 64)
    return jnp.concatenate([low, high], axis=1)


def on_device(hidden, policy_head, reference_head, targets, loss_mask):
    x, y, z, core = (lax.axis_index(name) for name in ("x", "y", "z", "core"))
    rows = policy_head.shape[0]
    heads = [policy_head, reference_head]
    heads += [shifted(head, "core", 1) for head in heads]
    numbers = jnp.stack(
        [
            (((y * 8 + z) * 2 + core) * 4 + x) * rows,
            (((y * 8 + z) * 2 + 1 - core) * 4 + x) * rows,
            y,
            (y + 1) % 4,
            (y + 3) % 4,
            (y + 2) % 4,
            x,
            (x + 1) % 4,
            (x + 3) % 4,
            (x + 2) % 4,
        ]
    ).astype(jnp.int32)
    mine = lambda array: lax.dynamic_index_in_dim(
        array.reshape(4, 4, 8, 2, 4), core, axis=3, keepdims=False
    )
    wanted = by_slot(mine(targets))
    weights = by_slot(mine(loss_mask)).astype(jnp.float32)

    own = hidden[0]
    up = {k: shifted(own, "z", k) for k in (2, -2, 1, -1)}
    up[4], up[3], up[5] = shifted(up[2], "z", 2), shifted(up[2], "z", 1), shifted(up[-2], "z", -1)
    up[0], up[6], up[7] = own, up[-2], up[-1]
    low, high = ordered_z([up[k] for k in range(8)], z)
    one = ordered([low] + [shifted(low, "x", k) for k in (1, 2, 3)], x)
    two = ordered([high] + [shifted(high, "y", k) for k in (1, 2, 3)], y)

    one_up, one_down = [shifted(one[0], "y", 1)], [shifted(one[1], "y", -1)]
    two_up, two_down = [shifted(two[0], "x", 1)], [shifted(two[1], "x", -1)]
    one_up.append(shifted(one[1], "y", 1))
    one_down.append(shifted(one[0], "y", -1))
    two_up.append(shifted(two[1], "x", 1))
    two_down.append(shifted(two[0], "x", -1))
    one_far = [shifted(one_up[0], "y", 1), shifted(one_down[0], "y", -1)]
    two_far = [shifted(two_up[0], "x", 1), shifted(two_down[0], "x", -1)]

    early = ((2, 0), (2, 32), (6, 64), (6, 96), (3, 0), (4, 32), (7, 64), (8, 96))
    late = ((3, 32), (4, 0), (7, 96), (8, 64), (5, 0), (5, 32), (9, 64), (9, 96))
    pieces = [*one, *two, one_up[0], one_down[0], two_up[0], two_down[0]]
    moments, *heads = moments_call(early, pieces, heads, numbers, wanted, None, 1)
    pieces = [one_up[1], one_down[1], two_up[1], two_down[1], *one_far, *two_far]
    (moments,) = moments_call(late, pieces, heads, numbers, wanted, moments, 16)

    moments = combined(received(moments, ("y", "x")), 8)
    here = finished(received(moments, "z"), weights)
    there = shifted(here, "core", 1)
    logprob, divergence, totals = placed(here, there, core, targets.size)
    return logprob, divergence, totals


def solution(mesh):
    torus = Mesh(mesh.devices.reshape(4, 8, 2, 4), ROWS)
    placed = (P("x", ("y", "z", "core"), None), P(ROWS, None), P(ROWS, None), P(), P())
    return jax.shard_map(
        on_device, mesh=torus, in_specs=placed, out_specs=(P(), P(), P()), check_vma=False
    )
```
